32 devices in a mesh: member: 2 (over y), blk: 16 (over z, x, core).
Axes of the slice: x: 2, y: 2, z: 4, core: 2. Of those that a mesh axis runs over, the one named last changes fastest.
Arguments:
- pressure: float32 [55, 8192], P(None, ('member', 'blk')), parts along dimension 1, may hold values from -6 to 6
- velocity: float32 [55, 24576], P(None, ('member', 'blk')), parts along dimension 1, may hold values from -3 to 3
- tracers: float32 [3, 55, 8192], P(None, None, ('member', 'blk')), parts along dimension 2, may hold values from 0.1 to 2
- tendency: float32 [55, 8192], P(None, ('member', 'blk')), parts along dimension 1, may hold values from -6 to 6
- pattern: float32 [8192], P(('member', 'blk')), parts along dimension 0, may hold values from -0.9 to 0.9
- coupling: float32 [55, 4096], P(None, 'blk'), may hold values from 0.3 to 3
- edge_length: float32 [12288], P('blk'), may hold values from 0.7 to 1.4
- inv_distance: float32 [12288], P('blk'), may hold values from 0.7 to 1.4
- inv_area: float32 [4096], P('blk'), may hold values from 0.7 to 1.4
- edge_ends: int32 [2, 12288], P(None, 'blk'), may hold values from 0 to 351, as said below
- halo_ends: int32 [2, 2048], P(None, 'blk'), may hold values from 0 to 351, as said below
- cell_edges: int32 [8, 4096], P(None, 'blk'), may hold values from 0 to 895, as said below
- cell_signs: int32 [8, 4096], P(None, 'blk'), may hold values from -1 to 1, as said below
- cell_send: int32 [6, 256], P(None, 'blk'), may hold values from 0 to 255, as said below
- edge_send: int32 [4, 512], P(None, 'blk'), may hold values from 0 to 767, as said below
Outputs:
- new_pressure: float32 [55, 8192], P(None, ('member', 'blk')), parts along dimension 1
- new_velocity: float32 [55, 24576], P(None, ('member', 'blk')), parts along dimension 1
- new_tracers: float32 [3, 55, 8192], P(None, None, ('member', 'blk')), parts along dimension 2
The draws below stay inside these ranges and needn't reach their ends.
There are 2 independent parts, one for each index of `member`. The reference program is written for one: setup_inputs(seed, part) draws one part's arguments, and reference() takes and returns one part's arrays. A program takes and returns all parts, laid end to end along the dimension named above; an argument that names none is the same for every part. Nothing has to cross between parts.
Inputs may be any that keep to these rules, and one draw needn't show every extreme that they name: `cell_send`: the cells form a periodic hexagonal lattice; each device holds a 16 x 16 patch, numbered in a drawn order; a patch touches the patches of the devices at index offsets 1, -1, 4, -4, 3 and 1 - 4 (modulo 16). Row k of a device's block lists the own cells that the device at index + o_k receives, o = (1, -1, 4, -4, 3, 1 - 4); rows 0 to 3 hold 16 live entries, rows 4 and 5 one live entry first, the rest repeat it. `edge_send`: row k of a device's block lists the own edges that the device at index + p_k receives, p = (1, 4, -4, 1 - 4); the live entries come first, 31, 16, 15 and 1 of them, the rest repeat a live one. `edge_ends`: row 0 is an own cell; row 1 is the neighbouring cell, own or received; the numbering is consistent with cell_send. `halo_ends`: for live received slots, the owner's edge's start and end as the receiver numbers them; other slots hold cells that no output reads. `cell_edges`: each own cell lists its six edges once each, in a drawn order, and two unused entries, whose sign is 0. `cell_signs`: 1 where the cell is the edge's start, -1 where it is its end, 0 on the unused entries.
All inputs are finite; a program needn't handle non-finite values.
Results may differ from the reference program's by a relative error of at most 0.0003.
Values sent between devices are 32-bit elements; how exact they have to be, the bound alone decides.
A program may use at most 128 MiB of HBM per device.

```python
import math
import jax
import jax.numpy as jnp
import numpy as np

B = 16
L = 55
NT = 3
SUBSTEPS = 6
BROW = 4
ALL_CELLS = 4096
ALL_EDGES = 12288
N_BLK = 16


def neighbour(across, upward, shift_a, shift_b):
    moved_a = across + shift_a
    moved_b = upward + shift_b
    block_a = np.where(moved_a >= B, 1, np.where(moved_a < 0, -1, 0))
    block_b = np.where(moved_b >= B, 1, np.where(moved_b < 0, -1, 0))
    return (block_a, block_b, moved_a - block_a * B, moved_b - block_b * B)


def cell_slot(block_a, block_b, moved_a, moved_b):
    peer_row = np.where((block_a == -1) & (block_b == 0), 0, np.where((block_a == 1) & (block_b == 0), 1, np.where((block_a == 0) & (block_b == -1), 2, np.where((block_a == 0) & (block_b == 1), 3, np.where((block_a == 1) & (block_b == -1), 4, 5)))))
    within = np.where(peer_row < 2, moved_b, np.where(peer_row < 4, moved_a, 0))
    return B * B + peer_row * B + within


def static_layout():
    own_cells = B * B
    own_edges = 3 * B * B
    lattice = np.arange(own_cells)
    across = lattice % B
    upward = lattice // B
    steps_a = (1, 0, 1)
    steps_b = (0, 1, -1)
    end_inside = []
    end_lattice = []
    end_slot = []
    slot_inside = []
    slot_lattice = []
    slot_index = []
    slot_sign = []
    for direction in range(3):
        block_a, block_b, moved_a, moved_b = neighbour(across, upward, steps_a[direction], steps_b[direction])
        inside = (block_a == 0) & (block_b == 0)
        end_inside.append(inside)
        end_lattice.append(moved_a + B * moved_b)
        end_slot.append(cell_slot(block_a, block_b, moved_a, moved_b))
        slot_inside.append(np.ones(own_cells, bool))
        slot_lattice.append(direction * own_cells + lattice)
        slot_index.append(np.zeros(own_cells, np.int64))
        slot_sign.append(np.ones(own_cells, np.int64))
    for direction in range(3):
        block_a, block_b, moved_a, moved_b = neighbour(across, upward, -steps_a[direction], -steps_b[direction])
        inside = (block_a == 0) & (block_b == 0)
        peer_row = np.where((block_a == -1) & (block_b == 0), 0, np.where((block_a == 0) & (block_b == -1), 1, np.where((block_a == 0) & (block_b == 1), 2, 3)))
        if direction == 0:
            first_within = moved_b
        else:
            first_within = B + moved_b - 1
        within = np.where(peer_row == 0, first_within, np.where(peer_row < 3, moved_a, 0))
        slot_inside.append(inside)
        slot_lattice.append(direction * own_cells + moved_a + B * moved_b)
        slot_index.append(own_edges + peer_row * 2 * B + within)
        slot_sign.append(-np.ones(own_cells, np.int64))
    for padding in range(2):
        slot_inside.append(np.ones(own_cells, bool))
        slot_lattice.append(np.zeros(own_cells, np.int64))
        slot_index.append(np.zeros(own_cells, np.int64))
        slot_sign.append(np.zeros(own_cells, np.int64))
    within = np.arange(B)
    cell_rows = np.stack([B - 1 + B * within, B * within, within + B * (B - 1), within, np.full(B, B * (B - 1)), np.full(B, B - 1)])
    double = np.arange(2 * B)
    row_zero = np.where(double < B, B - 1 + B * np.minimum(double, B - 1), np.where(double < 2 * B - 1, 2 * own_cells + B - 1 + B * np.clip(double - B + 1, 0, B - 1), B - 1))
    row_one = np.where(double < B, own_cells + np.minimum(double, B - 1) + B * (B - 1), own_cells + B * (B - 1))
    row_two = np.where(double < B - 1, 2 * own_cells + np.minimum(double, B - 1), 2 * own_cells)
    row_three = np.full(2 * B, 2 * own_cells + B - 1)
    edge_rows = np.stack([row_zero, row_one, row_two, row_three])
    start_zero = np.where(double < B, own_cells + double, np.where(double < 2 * B - 1, own_cells + double - B + 1, 0))
    end_zero = np.where(double < B, B * double, np.where(double < 2 * B - 1, B * (double - B), 0))
    start_one = np.where(double < B, own_cells + 2 * B + double, 0)
    end_one = np.where(double < B, double, 0)
    start_two = np.where(double < B - 1, own_cells + 3 * B + double, 0)
    end_two = np.where(double < B - 1, double + 1 + B * (B - 1), 0)
    start_three = np.where(double < 1, own_cells + 5 * B, 0)
    end_three = np.where(double < 1, B * (B - 1), 0)
    halo_start = np.concatenate([start_zero, start_one, start_two, start_three])
    halo_end = np.concatenate([end_zero, end_one, end_two, end_three])
    return (np.concatenate(end_inside), np.concatenate(end_lattice).astype(np.int32), np.concatenate(end_slot).astype(np.int32), np.stack(slot_inside, axis=1), np.stack(slot_lattice, axis=1).astype(np.int32), np.stack(slot_index, axis=1).astype(np.int32), np.stack(slot_sign, axis=1).astype(np.int32), cell_rows.astype(np.int32), edge_rows.astype(np.int32), halo_start.astype(np.int32), halo_end.astype(np.int32))


def lattice_tables(key):
    own_cells = B * B
    own_edges = 3 * B * B
    end_inside, end_lattice, end_slot, slot_inside, slot_lattice, slot_index, slot_sign, cell_rows, edge_rows, halo_start, halo_end = static_layout()
    cell_order = jax.vmap(lambda single: jax.random.permutation(single, own_cells))(jax.random.split(jax.random.fold_in(key, 101), N_BLK)).astype(jnp.int32)
    edge_order = jax.vmap(lambda single: jax.random.permutation(single, own_edges))(jax.random.split(jax.random.fold_in(key, 102), N_BLK)).astype(jnp.int32)
    device = jnp.arange(N_BLK, dtype=jnp.int32)[:, None]
    start_local = cell_order[:, (np.arange(own_edges) % own_cells).astype(np.int32)]
    end_local = jnp.where(end_inside[None, :], cell_order[:, end_lattice], end_slot[None, :])
    ends_table = jnp.zeros((2, N_BLK, own_edges), jnp.int32).at[:, device, edge_order].set(jnp.stack([start_local, end_local]))
    edge_ends = ends_table.reshape(2, N_BLK * own_edges)
    halo_starts = jnp.broadcast_to(jnp.asarray(halo_start)[None, :], (N_BLK, 8 * B))
    halo_finish = cell_order[:, halo_end]
    halo_ends = jnp.stack([halo_starts, halo_finish]).reshape(2, N_BLK * 8 * B)
    slot_value = jnp.where(slot_inside[None], edge_order[:, slot_lattice], slot_index[None])
    sign_table = jnp.broadcast_to(jnp.asarray(slot_sign)[None], (N_BLK, own_cells, 8))
    scores = jax.random.randint(jax.random.fold_in(key, 103), (N_BLK, own_cells, 8), 0, 1 << 20) * 8 + jnp.arange(8, dtype=jnp.int32)
    shuffle = jnp.argsort(scores, axis=-1)
    slot_value = jnp.take_along_axis(slot_value, shuffle, axis=-1)
    sign_table = jnp.take_along_axis(sign_table, shuffle, axis=-1)
    placed = jnp.zeros((N_BLK, own_cells, 8), jnp.int32).at[device, cell_order].set(slot_value)
    placed_signs = jnp.zeros((N_BLK, own_cells, 8), jnp.int32).at[device, cell_order].set(sign_table)
    cell_edges = placed.transpose(2, 0, 1).reshape(8, N_BLK * own_cells)
    cell_signs = placed_signs.transpose(2, 0, 1).reshape(8, N_BLK * own_cells)
    cell_send = cell_order[:, cell_rows].transpose(1, 0, 2).reshape(6, N_BLK * B)
    edge_send = edge_order[:, edge_rows].transpose(1, 0, 2).reshape(4, N_BLK * 2 * B)
    return (edge_ends, halo_ends, cell_edges, cell_signs, cell_send, edge_send)


def draw_edge_ends(key, part):
    return lattice_tables(key)[0]


def draw_halo_ends(key, part):
    return lattice_tables(key)[1]


def draw_cell_edges(key, part):
    return lattice_tables(key)[2]


def draw_cell_signs(key, part):
    return lattice_tables(key)[3]


def draw_cell_send(key, part):
    return lattice_tables(key)[4]


def draw_edge_send(key, part):
    return lattice_tables(key)[5]


def shard_levels(stream_key, extent, cuts, least, top_value):
    def one(dim, blocks):
        steps = jax.random.uniform(jax.random.fold_in(jax.random.fold_in(stream_key, 6), dim), (blocks,), jnp.float32, least / len(cuts), top_value / len(cuts))
        return jnp.repeat(jnp.exp(steps), extent[dim] // blocks).reshape((-1,) + (1,) * (len(extent) - dim - 1))

    loudness = one(*cuts[0])
    for cut in cuts[1:]:
        loudness = loudness * one(*cut)
    return loudness


def scatter_about(stream_key, shape, scale, most, cuts=(), held_as=jnp.bfloat16):
    factor_of = shard_levels(stream_key, shape, cuts, -0.22, 0.18) if cuts else 1.0
    values = jax.random.normal(stream_key, shape, jnp.float32) * scale * factor_of
    return jnp.minimum(jnp.maximum(values, -most), most).astype(held_as)


def setup_inputs(seed: int = 0, part: int = 0) -> dict:
    seeds = jax.random.split(jax.random.key(seed), 16)
    own_keys = jax.random.split(jax.random.fold_in(seeds[15], part), 16)
    pressure = scatter_about(own_keys[0], (L, ALL_CELLS), 1.0, 6.0, ((1, 16),), jnp.float32)
    velocity = scatter_about(own_keys[1], (L, ALL_EDGES), 0.5, 3.0, ((1, 16),), jnp.float32)
    tracers = jnp.clip(jnp.exp(math.log(2.0) - 2.9957323 * jax.random.uniform(own_keys[2], (NT, L, ALL_CELLS), jnp.float32) ** shard_levels(own_keys[2], (NT, L, ALL_CELLS), ((2, 16),), -0.2, 0.2)), 0.1, 2.0)
    tendency = scatter_about(own_keys[3], (L, ALL_CELLS), 1.0, 6.0, ((1, 16),), jnp.float32)
    pattern = jnp.clip(jax.random.uniform(own_keys[4], (ALL_CELLS,), jnp.float32, -0.9, 0.9) * shard_levels(own_keys[4], (ALL_CELLS,), ((0, 16),), -0.4, 0.0), -0.9, 0.9)
    coupling = jnp.clip(jnp.exp(math.log(3.0) - 2.3025851 * jax.random.uniform(seeds[5], (L, ALL_CELLS), jnp.float32) ** shard_levels(seeds[5], (L, ALL_CELLS), ((1, 16),), -0.2, 0.2)), 0.3, 3.0)
    edge_length = jnp.clip(jnp.exp(math.log(1.4) - 0.6931472 * jax.random.uniform(seeds[6], (ALL_EDGES,), jnp.float32) ** shard_levels(seeds[6], (ALL_EDGES,), ((0, 16),), -0.2, 0.2)), 0.7, 1.4)
    inv_distance = jnp.clip(jnp.exp(math.log(1.4) - 0.6931472 * jax.random.uniform(seeds[7], (ALL_EDGES,), jnp.float32) ** shard_levels(seeds[7], (ALL_EDGES,), ((0, 16),), -0.2, 0.2)), 0.7, 1.4)
    inv_area = jnp.clip(jnp.exp(math.log(1.4) - 0.6931472 * jax.random.uniform(seeds[8], (ALL_CELLS,), jnp.float32) ** shard_levels(seeds[8], (ALL_CELLS,), ((0, 16),), -0.2, 0.2)), 0.7, 1.4)
    edge_ends = draw_edge_ends(jax.random.fold_in(seeds[15], 71), part)
    halo_ends = draw_halo_ends(jax.random.fold_in(seeds[15], 71), part)
    cell_edges = draw_cell_edges(jax.random.fold_in(seeds[15], 71), part)
    cell_signs = draw_cell_signs(jax.random.fold_in(seeds[15], 71), part)
    cell_send = draw_cell_send(jax.random.fold_in(seeds[15], 71), part)
    edge_send = draw_edge_send(jax.random.fold_in(seeds[15], 71), part)
    return dict(pressure=pressure, velocity=velocity, tracers=tracers, tendency=tendency, pattern=pattern, coupling=coupling, edge_length=edge_length, inv_distance=inv_distance, inv_area=inv_area, edge_ends=edge_ends, halo_ends=halo_ends, cell_edges=cell_edges, cell_signs=cell_signs, cell_send=cell_send, edge_send=edge_send)


grad_scale = 0.25
spread_scale = 0.25
force_scale = 0.5
tracer_scale = 0.05


def vertical_taper(levels):
    height = jnp.arange(levels, dtype=jnp.float32)
    return jnp.minimum(1.0, (levels - 1.0 - height) / (0.25 * levels))


def factor_columns(coupling):
    levels = coupling.shape[0]
    upper_link = jnp.concatenate([coupling[1:], jnp.zeros_like(coupling[:1])], axis=0)
    diagonal = 1.0 + coupling + upper_link
    inverses = []
    ratios = []
    for height in range(levels):
        if height == 0:
            divisor = diagonal[0]
        else:
            divisor = diagonal[height] + coupling[height] * ratios[-1]
        inverse = 1.0 / divisor
        inverses.append(inverse)
        ratios.append(-upper_link[height] * inverse)
    return jnp.stack(inverses), jnp.stack(ratios)


def solve_columns(source, coupling, inverses, ratios):
    levels = source.shape[0]
    forward = [source[0] * inverses[0]]
    for height in range(1, levels):
        forward.append((source[height] + coupling[height] * forward[-1]) * inverses[height])
    result = [forward[-1]]
    for height in range(levels - 2, -1, -1):
        result.append(forward[height] - ratios[height] * result[-1])
    return jnp.stack(result[::-1])


def extended_maps(cell_send, edge_send):
    own_cells = B * B
    own_edges = 3 * B * B
    cell_offsets = jnp.array([1, -1, BROW, -BROW, BROW - 1, 1 - BROW], dtype=jnp.int32)
    edge_offsets = jnp.array([1, BROW, -BROW, 1 - BROW], dtype=jnp.int32)
    device = jnp.arange(N_BLK, dtype=jnp.int32)[:, None]
    position = jnp.arange(own_cells + 6 * B, dtype=jnp.int32)[None, :]
    peer_row = jnp.clip((position - own_cells) // B, 0, 5)
    within = (position - own_cells) % B
    source = (device - cell_offsets[peer_row]) % N_BLK
    remote = source * own_cells + cell_send[peer_row, source * B + within]
    cell_map = jnp.where(position < own_cells, device * own_cells + position, remote)
    position = jnp.arange(own_edges + 8 * B, dtype=jnp.int32)[None, :]
    peer_row = jnp.clip((position - own_edges) // (2 * B), 0, 3)
    within = (position - own_edges) % (2 * B)
    source = (device - edge_offsets[peer_row]) % N_BLK
    remote = source * own_edges + edge_send[peer_row, source * (2 * B) + within]
    edge_map = jnp.where(position < own_edges, device * own_edges + position, remote)
    return cell_map.astype(jnp.int32), edge_map.astype(jnp.int32)


def reference(pressure, velocity, tracers, tendency, pattern, coupling, edge_length, inv_distance, inv_area, edge_ends, halo_ends, cell_edges, cell_signs, cell_send, edge_send):
    own_cells = B * B
    own_edges = 3 * B * B
    cell_map, edge_map = extended_maps(cell_send, edge_send)
    local_ends = edge_ends.reshape(2, N_BLK, own_edges)
    start_global = jnp.take_along_axis(cell_map, local_ends[0], axis=1).reshape(-1)
    end_global = jnp.take_along_axis(cell_map, local_ends[1], axis=1).reshape(-1)
    all_ends = jnp.concatenate([local_ends, halo_ends.reshape(2, N_BLK, 8 * B)], axis=2)
    slot_edges = cell_edges.reshape(8, N_BLK, own_cells)
    edge_global = []
    first_global = []
    last_global = []
    weights = []
    for column_slot in range(8):
        chosen = slot_edges[column_slot]
        edge_global.append(jnp.take_along_axis(edge_map, chosen, axis=1).reshape(-1))
        first_global.append(jnp.take_along_axis(cell_map, jnp.take_along_axis(all_ends[0], chosen, axis=1), axis=1).reshape(-1))
        last_global.append(jnp.take_along_axis(cell_map, jnp.take_along_axis(all_ends[1], chosen, axis=1), axis=1).reshape(-1))
        weights.append(cell_signs[column_slot].astype(jnp.float32) * edge_length[edge_global[-1]] * inv_area)
    forcing = force_scale * (1.0 + pattern[None, :] * vertical_taper(L)[:, None]) * tendency
    inverses, ratios = factor_columns(coupling)
    current = pressure
    edge_flow = velocity
    flow_total = jnp.zeros_like(velocity)
    for substep in range(SUBSTEPS):
        edge_flow = edge_flow - grad_scale * inv_distance * (current[:, end_global] - current[:, start_global])
        flow_total = flow_total + edge_flow
        spread = weights[0] * edge_flow[:, edge_global[0]]
        for column_slot in range(1, 8):
            spread = spread + weights[column_slot] * edge_flow[:, edge_global[column_slot]]
        current = solve_columns(current - spread_scale * spread + forcing, coupling, inverses, ratios)
    mean_flow = flow_total * (1.0 / SUBSTEPS)
    tracer_spread = jnp.zeros_like(tracers)
    for column_slot in range(8):
        chosen_flow = mean_flow[:, edge_global[column_slot]]
        tracer_flux = jnp.maximum(chosen_flow, 0.0)[None] * tracers[:, :, first_global[column_slot]] + jnp.minimum(chosen_flow, 0.0)[None] * tracers[:, :, last_global[column_slot]]
        tracer_spread = tracer_spread + weights[column_slot] * tracer_flux
    new_tracers = tracers - tracer_scale * tracer_spread
    return current, edge_flow, new_tracers
```

```python
import functools

import jax
import jax.numpy as jnp
from jax import lax
from jax.experimental import pallas as pl
from jax.experimental.pallas import tpu as pltpu
from jax.sharding import PartitionSpec as P

SUBSTEPS = 6
grad_scale = 0.25
spread_scale = 0.25
force_scale = 0.5
tracer_scale = 0.05

F32 = jnp.float32
BF16 = jnp.bfloat16
MESH = pl.DeviceIdType.MESH
LANES = 128


def up_to(value, unit):
    return -(-value // unit) * unit


def dot(a, b):
    return jnp.dot(a, b, preferred_element_type=F32)


def halves(x):
    high = x.astype(BF16).astype(F32)
    return jnp.concatenate([high, x - high], axis=0).astype(BF16)


def fold(x):
    rows = x.shape[0] // 2
    return x[:rows] + x[rows:]


def pick(x, table):
    return fold(dot(halves(x), table))


def pad_rows(x, rows):
    if x.shape[0] == rows:
        return x
    return jnp.concatenate([x, jnp.zeros((rows - x.shape[0], x.shape[1]), x.dtype)], axis=0)


def pad_lanes(x, lanes, value=0):
    if x.shape[1] == lanes:
        return x
    return jnp.concatenate(
        [x, jnp.full((x.shape[0], lanes - x.shape[1]), value, x.dtype)], axis=1
    )


def one_hot(rows, index):
    where = lax.broadcasted_iota(jnp.int32, (rows, index.shape[1]), 0)
    return jnp.where(where == index, 1.0, 0.0)


def down(x, steps, fill=None):
    moved = pltpu.roll(x, steps, 0)
    if fill is None:
        return moved
    rows = lax.broadcasted_iota(jnp.int32, x.shape, 0)
    return jnp.where(rows < steps, fill, moved)


def up(x, steps, fill=None):
    moved = pltpu.roll(x, x.shape[0] - steps, 0)
    if fill is None:
        return moved
    rows = lax.broadcasted_iota(jnp.int32, x.shape, 0)
    return jnp.where(rows >= x.shape[0] - steps, fill, moved)


def strides(rows):
    found = []
    step = 1
    while step < rows:
        found.append(step)
        step *= 2
    return found


def factor_columns(c, levels, inv_ref, a_ref, b_ref):
    rows = c.shape[0]
    above = up(c, 1, 0.0)
    m = [1.0 + c, c, jnp.ones_like(c), c]
    for step in strides(rows):
        if step >= 16:
            scale = 1.0 / (m[0] + m[1] + m[2] + m[3])
            m = [entry * scale for entry in m]
        o = [
            down(m[0], step, 1.0),
            down(m[1], step, 0.0),
            down(m[2], step, 0.0),
            down(m[3], step, 1.0),
        ]
        m = [
            m[0] * o[0] + m[1] * o[2],
            m[0] * o[1] + m[1] * o[3],
            m[2] * o[0] + m[3] * o[2],
            m[2] * o[1] + m[3] * o[3],
        ]
    inverse = 1.0 / (above + m[0] / m[2])
    inv_ref[...] = inverse
    row = lax.broadcasted_iota(jnp.int32, c.shape, 0)
    a = jnp.where(row < 1, 0.0, c * inverse)
    b = jnp.where(row >= levels - 1, 0.0, above * inverse)
    for number, step in enumerate(strides(rows)):
        a_ref[number] = a
        b_ref[number] = b
        a = a * down(a, step, 0.0)
        b = b * up(b, step, 0.0)


def solve(source, lanes, inv_ref, a_ref, b_ref):
    y = source * inv_ref[:, lanes]
    steps = strides(source.shape[0])
    for number, step in enumerate(steps):
        y = y + a_ref[number, :, lanes] * down(y, step)
    for number, step in enumerate(steps):
        y = y + b_ref[number, :, lanes] * up(y, step)
    return y


def kernel(
    cell_offsets, edge_offsets,
    p_ref, u_ref, t_ref, tend_ref, pat_ref, coup_ref, len_ref, dist_ref, area_ref,
    ends_ref, hends_ref, ce_ref, cs_ref, csend_ref, esend_ref,
    p_out, u_out, t_out,
    send0, recv0, esend, erecv, sends, recvs,
    gs_ref, ge_ref, gc_ref, d_ref, wh_ref, wl_ref, a_ref, b_ref, inv_ref, trs_ref, tre_ref,
    send0_sem, recv0_sem, esend_sem, erecv_sem, sends_sem, recvs_sem,
):
    count = lax.axis_size("blk")
    member = lax.axis_index("member")
    me = lax.axis_index("blk")

    def peer(offset):
        return (member, lax.rem(me + (offset + count), count))

    barrier = pltpu.get_barrier_semaphore()
    for offset in cell_offsets:
        pl.semaphore_signal(barrier, inc=1, device_id=peer(offset), device_id_type=MESH)

    levels, own = p_ref.shape
    species = t_ref.shape[0]
    owned = u_ref.shape[1]
    peers, slots = csend_ref.shape
    epeers, eslots = esend_ref.shape
    rows = up_to(levels, 8)
    rim = up_to(peers * slots, LANES)
    hal = peers * slots
    ehal = epeers * eslots
    OWN = slice(0, own)
    RIM = slice(own, own + rim)

    csend = jnp.concatenate([csend_ref[k : k + 1, :] for k in range(peers)], axis=1)
    sel = one_hot(own, pad_lanes(csend, rim, -1)).astype(BF16)
    esel_row = jnp.concatenate([esend_ref[k : k + 1, :] for k in range(epeers)], axis=1)
    esel = one_hot(owned, esel_row).astype(BF16)

    pressure = pad_rows(p_ref[...], rows)
    tracers = [pad_rows(t_ref[s], rows) for s in range(species)]
    coupling = pad_rows(coup_ref[...], rows)
    height = lax.broadcasted_iota(jnp.int32, (levels, own), 0).astype(F32)
    taper = jnp.minimum(1.0, (levels - 1.0 - height) / (0.25 * levels))
    forcing = pad_rows(force_scale * (1.0 + pat_ref[...] * taper) * tend_ref[...], rows)
    area = area_ref[...]
    area8 = pad_rows(area, 8)
    sent = pick(jnp.concatenate([pressure] + tracers, axis=0), sel)
    wide = send0.shape[1]
    send0[...] = jnp.transpose(pad_rows(sent, wide))[:hal]
    edges = jnp.concatenate(
        [pad_rows(u_ref[...], rows), len_ref[...], dist_ref[...], jnp.zeros((6, owned), F32)],
        axis=0,
    )
    esend[...] = jnp.transpose(pad_rows(pick(edges, esel), LANES))

    pl.semaphore_wait(barrier, len(cell_offsets))
    first = []
    for k, offset in enumerate(cell_offsets):
        copy = pltpu.make_async_remote_copy(
            src_ref=send0.at[pl.ds(k * slots, slots)],
            dst_ref=recv0.at[pl.ds(k * slots, slots)],
            send_sem=send0_sem.at[k],
            recv_sem=recv0_sem.at[k],
            device_id=peer(offset),
            device_id_type=MESH,
        )
        copy.start()
        first.append(copy)
    efirst = []
    for k, offset in enumerate(edge_offsets):
        copy = pltpu.make_async_remote_copy(
            src_ref=esend.at[pl.ds(k * eslots, eslots)],
            dst_ref=erecv.at[pl.ds(k * eslots, eslots)],
            send_sem=esend_sem.at[k],
            recv_sem=erecv_sem.at[k],
            device_id=peer(offset),
            device_id_type=MESH,
        )
        copy.start()
        efirst.append(copy)

    column = jnp.concatenate([coupling, forcing, area8], axis=0)
    column_rim = pick(column, sel)
    force_own, force_rim = forcing, column_rim[rows : 2 * rows]
    area_rim = column_rim[2 * rows : 2 * rows + 1]
    area_all = jnp.concatenate([area, area_rim], axis=1)
    factor_columns(
        jnp.concatenate([coupling, column_rim[:rows]], axis=1), levels, inv_ref, a_ref, b_ref
    )

    start = jnp.concatenate([ends_ref[0:1, :], hends_ref[0:1, :]], axis=1)
    end = jnp.concatenate([ends_ref[1:2, :], hends_ref[1:2, :]], axis=1)
    ext = own + rim
    gs_ref[...] = one_hot(ext, start).astype(BF16)
    ge_ref[...] = one_hot(ext, end).astype(BF16)
    total = owned + ehal
    where = lax.broadcasted_iota(jnp.int32, (total, own), 0)
    table = jnp.zeros((total, own), F32)
    for j in range(ce_ref.shape[0]):
        sign = cs_ref[j : j + 1, :]
        index = jnp.where(sign == 0, -1, ce_ref[j : j + 1, :])
        table = jnp.where(where == index, sign.astype(F32), table)
    d_ref[:, OWN] = table.astype(BF16)
    d_ref[:, RIM] = dot(d_ref[:, OWN], sel).astype(BF16)

    for copy in efirst:
        copy.wait_recv()
    edges = jnp.concatenate([edges, jnp.transpose(erecv[...])[: edges.shape[0]]], axis=1)
    velocity = edges[:rows]
    length = edges[rows : rows + 1]
    distance = edges[rows + 1 : rows + 2]
    conduct = (spread_scale * grad_scale) * length * distance
    conduct_high = conduct.astype(BF16).astype(F32)
    gd = ge_ref[...].astype(F32) - gs_ref[...].astype(F32)
    gc_ref[:ext] = (gd * conduct_high).astype(BF16)
    gc_ref[ext:] = (gd * (conduct - conduct_high)).astype(BF16)
    weight = fold(dot(gc_ref[...], d_ref[...])) * area_all
    weight_high = weight.astype(BF16)
    wh_ref[...] = weight_high
    wl_ref[...] = (weight - weight_high.astype(F32)).astype(BF16)
    spread = pick(velocity * length, d_ref[...]) * (spread_scale * area_all)
    q_own, q_rim = spread[:, OWN], spread[:, RIM]

    for copy in first:
        copy.wait_recv()
    arrived = jnp.transpose(pad_rows(recv0[...], rim))
    halo = arrived[:rows]
    tracer_ext = jnp.concatenate(
        [
            jnp.concatenate([tracers[s], arrived[(s + 1) * rows : (s + 2) * rows]], axis=1)
            for s in range(species)
        ],
        axis=0,
    )

    def through(x, rows_of, lanes):
        parts = halves(x)
        return fold(dot(parts, wh_ref[rows_of, lanes])) + dot(
            parts[: x.shape[0]], wl_ref[rows_of, lanes]
        )

    p_own, p_rim = pressure, sent[:rows]
    sum_one = jnp.zeros((rows, ext), F32)
    sum_two = jnp.zeros((rows, ext), F32)
    lap_own = through(p_own, OWN, slice(0, ext))
    pending = []
    for n in range(SUBSTEPS):
        last = n == SUBSTEPS - 1
        now = jnp.concatenate([p_own, halo], axis=1)
        if not last:
            q_rim = q_rim - (lap_own[:, RIM] + through(halo, RIM, RIM))
            p_rim = solve(p_rim - q_rim + force_rim, RIM, inv_ref, a_ref, b_ref)
            sends[n] = jnp.transpose(pad_rows(p_rim, LANES))[:hal]
            copies = []
            for k, offset in enumerate(cell_offsets):
                copy = pltpu.make_async_remote_copy(
                    src_ref=sends.at[n, pl.ds(k * slots, slots)],
                    dst_ref=recvs.at[n, pl.ds(k * slots, slots)],
                    send_sem=sends_sem.at[n, k],
                    recv_sem=recvs_sem.at[n, k],
                    device_id=peer(offset),
                    device_id_type=MESH,
                )
                copy.start()
                copies.append(copy)
            pending += copies
        q_own = q_own - (lap_own[:, OWN] + through(halo, RIM, OWN))
        p_own = solve(p_own - q_own + force_own, OWN, inv_ref, a_ref, b_ref)
        if not last:
            sum_one = sum_one + now
            sum_two = sum_two + (SUBSTEPS - n) * now
            lap_own = through(p_own, OWN, slice(0, ext))
            if n == 0:
                trs_ref[...] = pick(tracer_ext, gs_ref[...])
            if n == 1:
                tre_ref[...] = pick(tracer_ext, ge_ref[...])
            if n == SUBSTEPS - 2:
                table = (ge_ref[...].astype(F32) - gs_ref[...].astype(F32)).astype(BF16)
                both = pick(jnp.concatenate([sum_one, sum_two], axis=0), table)
                slope = grad_scale * distance
                flow = velocity - slope * both[:rows]
                gathered = SUBSTEPS * velocity - slope * both[rows:]
                gs_ref[...] = table
            for copy in copies:
                copy.wait_recv()
            halo = jnp.transpose(pad_rows(recvs[n], rim))[:rows]
        else:
            p_out[...] = p_own[:levels]
            change = (grad_scale * distance) * pick(now, gs_ref[...])
            u_out[...] = (flow - change)[:levels, :owned]
            mean = (gathered - change) * (1.0 / SUBSTEPS) * length
            ahead = jnp.maximum(mean, 0.0)
            back = jnp.minimum(mean, 0.0)
            for s in range(species):
                part = slice(s * rows, (s + 1) * rows)
                flux = ahead * trs_ref[part] + back * tre_ref[part]
                change = pick(flux, d_ref[:, OWN]) * (tracer_scale * area)
                t_out[s] = (tracers[s] - change)[:levels]
    for copy in first + efirst + pending:
        copy.wait_send()


def per_device(
    pressure, velocity, tracers, tendency, pattern, coupling, edge_length, inv_distance,
    inv_area, edge_ends, halo_ends, cell_edges, cell_signs, cell_send, edge_send,
):
    stride = max(4, lax.axis_size("blk") // 16)
    cell_offsets = (1, -1, stride, -stride, stride - 1, 1 - stride)
    edge_offsets = (1, stride, -stride, 1 - stride)
    levels, own = pressure.shape
    species = tracers.shape[0]
    owned = velocity.shape[1]
    peers, slots = cell_send.shape
    epeers, eslots = edge_send.shape
    rows = up_to(levels, 8)
    hal = peers * slots
    rim = up_to(hal, LANES)
    ehal = epeers * eslots
    ext, total = own + rim, owned + ehal
    wide = up_to((species + 1) * rows, LANES)
    steps = len(strides(rows))
    sem = pltpu.SemaphoreType.DMA
    vmem = pl.BlockSpec(memory_space=pltpu.VMEM)
    rounds = SUBSTEPS - 1
    return pl.pallas_call(
        functools.partial(kernel, cell_offsets, edge_offsets),
        out_shape=(
            jax.ShapeDtypeStruct(pressure.shape, F32),
            jax.ShapeDtypeStruct(velocity.shape, F32),
            jax.ShapeDtypeStruct(tracers.shape, F32),
        ),
        in_specs=[vmem] * 15,
        out_specs=(vmem, vmem, vmem),
        scratch_shapes=[
            pltpu.VMEM((hal, wide), F32),
            pltpu.VMEM((hal, wide), F32),
            pltpu.VMEM((ehal, LANES), F32),
            pltpu.VMEM((ehal, LANES), F32),
            pltpu.VMEM((rounds, hal, LANES), F32),
            pltpu.VMEM((rounds, hal, LANES), F32),
            pltpu.VMEM((ext, total), BF16),
            pltpu.VMEM((ext, total), BF16),
            pltpu.VMEM((2 * ext, total), BF16),
            pltpu.VMEM((total, ext), BF16),
            pltpu.VMEM((ext, ext), BF16),
            pltpu.VMEM((ext, ext), BF16),
            pltpu.VMEM((steps, rows, ext), F32),
            pltpu.VMEM((steps, rows, ext), F32),
            pltpu.VMEM((rows, ext), F32),
            pltpu.VMEM((species * rows, total), F32),
            pltpu.VMEM((species * rows, total), F32),
            sem((peers,)),
            sem((peers,)),
            sem((epeers,)),
            sem((epeers,)),
            sem((rounds, peers)),
            sem((rounds, peers)),
        ],
        compiler_params=pltpu.CompilerParams(collective_id=0, has_side_effects=True),
    )(
        pressure, velocity, tracers, tendency, pattern.reshape(1, -1), coupling,
        edge_length.reshape(1, -1), inv_distance.reshape(1, -1), inv_area.reshape(1, -1),
        edge_ends, halo_ends, cell_edges, cell_signs, cell_send, edge_send,
    )


def solution(mesh):
    both = ("member", "blk")
    in_specs = (
        P(None, both), P(None, both), P(None, None, both), P(None, both), P(both),
        P(None, "blk"), P("blk"), P("blk"), P("blk"),
        P(None, "blk"), P(None, "blk"), P(None, "blk"), P(None, "blk"), P(None, "blk"),
        P(None, "blk"),
    )
    out_specs = (P(None, both), P(None, both), P(None, None, both))
    return jax.shard_map(
        per_device, mesh=mesh, in_specs=in_specs, out_specs=out_specs, check_vma=False
    )
```

```python
import functools

import jax
import jax.numpy as jnp
from jax import lax
from jax.experimental import pallas as pl
from jax.experimental.pallas import tpu as pltpu
from jax.sharding import PartitionSpec as P

SUBSTEPS = 6
grad_scale = 0.25
spread_scale = 0.25
force_scale = 0.5
tracer_scale = 0.05

F32 = jnp.float32
BF16 = jnp.bfloat16
MESH = pl.DeviceIdType.MESH
LANES = 128


def up_to(value, unit):
    return -(-value // unit) * unit


def dot(a, b):
    return jnp.dot(a, b, preferred_element_type=F32)


def halves(x):
    high = x.astype(BF16).astype(F32)
    return jnp.concatenate([high, x - high], axis=0).astype(BF16)


def fold(x):
    rows = x.shape[0] // 2
    return x[:rows] + x[rows:]


def pick(x, table):
    return fold(dot(halves(x), table))


def pad_rows(x, rows):
    if x.shape[0] == rows:
        return x
    return jnp.concatenate([x, jnp.zeros((rows - x.shape[0], x.shape[1]), x.dtype)], axis=0)


def pad_lanes(x, lanes, value=0):
    if x.shape[1] == lanes:
        return x
    return jnp.concatenate(
        [x, jnp.full((x.shape[0], lanes - x.shape[1]), value, x.dtype)], axis=1
    )


def row(x):
    return jnp.concatenate([x[k : k + 1, :] for k in range(x.shape[0])], axis=1)


def halo_order(index, own, slots, rim):
    half = slots // 2
    shift = half.bit_length() - 1
    slot = index - own
    upper = (slot >> shift) & 1
    moved = ((slot >> (shift + 1)) << shift) + (slot & (half - 1)) + upper * (rim // 2)
    return jnp.where(index < own, index, own + moved)


def one_hot(rows, index):
    where = lax.broadcasted_iota(jnp.int32, (rows, index.shape[1]), 0)
    return jnp.where(where == index, 1.0, 0.0)


def down(x, steps, fill=None):
    moved = pltpu.roll(x, steps, 0)
    if fill is None:
        return moved
    rows = lax.broadcasted_iota(jnp.int32, x.shape, 0)
    return jnp.where(rows < steps, fill, moved)


def up(x, steps, fill=None):
    moved = pltpu.roll(x, x.shape[0] - steps, 0)
    if fill is None:
        return moved
    rows = lax.broadcasted_iota(jnp.int32, x.shape, 0)
    return jnp.where(rows >= x.shape[0] - steps, fill, moved)


def strides(rows):
    found = []
    step = 1
    while step < rows:
        found.append(step)
        step *= 2
    return found


def factor_columns(c, levels, lanes, inv_ref, a_ref, b_ref):
    rows = c.shape[0]
    above = up(c, 1, 0.0)
    m = [1.0 + c, c, jnp.ones_like(c), c]
    for step in strides(rows):
        if step >= 16:
            scale = 1.0 / (m[0] + m[1] + m[2] + m[3])
            m = [entry * scale for entry in m]
        o = [
            down(m[0], step, 1.0),
            down(m[1], step, 0.0),
            down(m[2], step, 0.0),
            down(m[3], step, 1.0),
        ]
        m = [
            m[0] * o[0] + m[1] * o[2],
            m[0] * o[1] + m[1] * o[3],
            m[2] * o[0] + m[3] * o[2],
            m[2] * o[1] + m[3] * o[3],
        ]
    inverse = 1.0 / (above + m[0] / m[2])
    inv_ref[:, lanes] = inverse
    height = lax.broadcasted_iota(jnp.int32, c.shape, 0)
    a = jnp.where(height < 1, 0.0, c * inverse)
    b = jnp.where(height >= levels - 1, 0.0, above * inverse)
    for number, step in enumerate(strides(rows)):
        a_ref[number, :, lanes] = a
        b_ref[number, :, lanes] = b
        a = a * down(a, step, 0.0)
        b = b * up(b, step, 0.0)


def solve(source, lanes, inv_ref, a_ref, b_ref):
    y = source * inv_ref[:, lanes]
    steps = strides(source.shape[0])
    for number, step in enumerate(steps):
        y = y + a_ref[number, :, lanes] * down(y, step)
    for number, step in enumerate(steps):
        y = y + b_ref[number, :, lanes] * up(y, step)
    return y


def kernel(
    cell_offsets, edge_offsets,
    p_hbm, u_hbm, t_hbm, tend_hbm, pat_hbm, coup_hbm, len_hbm, dist_hbm, area_hbm,
    ends_hbm, hends_hbm, ce_hbm, cs_hbm, csend_hbm, esend_hbm,
    p_out, u_out, t_out,
    send0, recv0, esend, erecv, sends, recvs,
    gs_ref, ge_ref, gc_ref, d_ref, wh_ref, wl_ref, a_ref, b_ref, inv_ref, trs_ref, tre_ref,
    p_ref, u_ref, t_ref, tend_ref, pat_ref, coup_ref, len_ref, dist_ref, area_ref,
    ends_ref, hends_ref, ce_ref, cs_ref, csend_ref, esend_ref,
    load_sem, send0_sem, recv0_sem, esend_sem, erecv_sem, sends_sem, recvs_sem,
):
    count = lax.axis_size("blk")
    member = lax.axis_index("member")
    me = lax.axis_index("blk")

    def peer(offset):
        return (member, lax.rem(me + (offset + count), count))

    barrier = pltpu.get_barrier_semaphore()
    for offset in cell_offsets:
        pl.semaphore_signal(barrier, inc=1, device_id=peer(offset), device_id_type=MESH)

    groups = (
        ((csend_hbm, csend_ref), (p_hbm, p_ref), (t_hbm, t_ref)),
        ((esend_hbm, esend_ref), (u_hbm, u_ref), (len_hbm, len_ref), (dist_hbm, dist_ref)),
        ((coup_hbm, coup_ref), (tend_hbm, tend_ref), (pat_hbm, pat_ref), (area_hbm, area_ref)),
        ((ends_hbm, ends_ref), (hends_hbm, hends_ref), (ce_hbm, ce_ref), (cs_hbm, cs_ref)),
    )
    loads = []
    for group in groups:
        loads.append([])
        for source, target in group:
            number = sum(len(ready) for ready in loads)
            copy = pltpu.make_async_copy(source, target, load_sem.at[number])
            copy.start()
            loads[-1].append(copy)

    def ready(number):
        for copy in loads[number]:
            copy.wait()

    levels, own = p_ref.shape
    species = t_ref.shape[0]
    owned = u_ref.shape[1]
    peers, slots = csend_ref.shape
    epeers, eslots = esend_ref.shape
    rows = up_to(levels, 8)
    rim = up_to(peers * slots, LANES)
    hal = peers * slots
    ehal = epeers * eslots
    OWN = slice(0, own)
    RIM = slice(own, own + rim)

    ready(0)
    csend = row(csend_ref[...])
    sel = one_hot(own, pad_lanes(csend, rim, -1)).astype(BF16)
    pressure = pad_rows(p_ref[...], rows)
    tracers = [pad_rows(t_ref[s], rows) for s in range(species)]
    sent = pick(jnp.concatenate([pressure] + tracers, axis=0), sel)
    wide = send0.shape[1]
    send0[...] = jnp.transpose(pad_rows(sent, wide))[:hal]
    ready(1)
    esel = one_hot(owned, row(esend_ref[...])).astype(BF16)
    edges = jnp.concatenate(
        [pad_rows(u_ref[...], rows), row(len_ref[...]), row(dist_ref[...]), jnp.zeros((6, owned), F32)],
        axis=0,
    )
    esend[...] = jnp.transpose(pad_rows(pick(edges, esel), LANES))

    pl.semaphore_wait(barrier, len(cell_offsets))
    first = []
    for k, offset in enumerate(cell_offsets):
        copy = pltpu.make_async_remote_copy(
            src_ref=send0.at[pl.ds(k * slots, slots)],
            dst_ref=recv0.at[pl.ds(k * slots, slots)],
            send_sem=send0_sem.at[k],
            recv_sem=recv0_sem.at[k],
            device_id=peer(offset),
            device_id_type=MESH,
        )
        copy.start()
        first.append(copy)
    efirst = []
    for k, offset in enumerate(edge_offsets):
        copy = pltpu.make_async_remote_copy(
            src_ref=esend.at[pl.ds(k * eslots, eslots)],
            dst_ref=erecv.at[pl.ds(k * eslots, eslots)],
            send_sem=esend_sem.at[k],
            recv_sem=erecv_sem.at[k],
            device_id=peer(offset),
            device_id_type=MESH,
        )
        copy.start()
        efirst.append(copy)

    ready(2)
    coupling = pad_rows(coup_ref[...], rows)
    height = lax.broadcasted_iota(jnp.int32, (levels, own), 0).astype(F32)
    taper = jnp.minimum(1.0, (levels - 1.0 - height) / (0.25 * levels))
    forcing = pad_rows(force_scale * (1.0 + row(pat_ref[...]) * taper) * tend_ref[...], rows)
    area = row(area_ref[...])
    area8 = pad_rows(area, 8)
    column = jnp.concatenate([coupling, forcing, area8], axis=0)
    column_rim = pick(column, sel)
    force_own, force_rim = forcing, column_rim[rows : 2 * rows]
    area_rim = column_rim[2 * rows : 2 * rows + 1]
    factor_columns(column_rim[:rows], levels, RIM, inv_ref, a_ref, b_ref)

    ready(3)
    start = jnp.concatenate([ends_ref[0:1, :], hends_ref[0:1, :]], axis=1)
    end = jnp.concatenate([ends_ref[1:2, :], hends_ref[1:2, :]], axis=1)
    start = halo_order(start, own, slots, rim)
    end = halo_order(end, own, slots, rim)
    ext = own + rim
    gs_ref[...] = one_hot(ext, start).astype(BF16)
    ge_ref[...] = one_hot(ext, end).astype(BF16)
    total = owned + ehal
    where = lax.broadcasted_iota(jnp.int32, (total, own), 0)
    table = jnp.zeros((total, own), F32)
    for j in range(ce_ref.shape[0]):
        sign = cs_ref[j : j + 1, :]
        index = jnp.where(sign == 0, -1, ce_ref[j : j + 1, :])
        table = jnp.where(where == index, sign.astype(F32), table)
    d_ref[:, OWN] = table.astype(BF16)
    d_ref[:, RIM] = dot(d_ref[:, OWN], sel).astype(BF16)

    for copy in efirst:
        copy.wait_recv()
    edges = jnp.concatenate([edges, jnp.transpose(erecv[...])[: edges.shape[0]]], axis=1)
    velocity = edges[:rows]
    length = edges[rows : rows + 1]
    distance = edges[rows + 1 : rows + 2]
    conduct = (spread_scale * grad_scale) * length * distance
    conduct_high = conduct.astype(BF16).astype(F32)
    gd = ge_ref[...].astype(F32) - gs_ref[...].astype(F32)
    gc_ref[:ext] = (gd * conduct_high).astype(BF16)
    gc_ref[ext:] = (gd * (conduct - conduct_high)).astype(BF16)
    flux = velocity * length

    def prepare(lanes, scale):
        weight = fold(dot(gc_ref[...], d_ref[:, lanes])) * scale
        weight_high = weight.astype(BF16)
        wh_ref[:, lanes] = weight_high
        wl_ref[:, lanes] = (weight - weight_high.astype(F32)).astype(BF16)
        return pick(flux, d_ref[:, lanes]) * (spread_scale * scale)

    q_rim = prepare(RIM, area_rim)

    for copy in first:
        copy.wait_recv()
    half = slots // 2
    lower = [recv0[k * slots : k * slots + half] for k in range(peers)]
    upper = [recv0[k * slots + half : (k + 1) * slots] for k in range(peers)]
    arrived = jnp.concatenate(
        [
            pad_rows(jnp.concatenate(lower, axis=0), rim // 2),
            pad_rows(jnp.concatenate(upper, axis=0), rim // 2),
        ],
        axis=0,
    )
    arrived = jnp.transpose(arrived)
    lane = lax.broadcasted_iota(jnp.int32, (rows, rim), 1)
    halo = arrived[:rows]
    tracer_ext = jnp.concatenate(
        [
            jnp.concatenate([tracers[s], arrived[(s + 1) * rows : (s + 2) * rows]], axis=1)
            for s in range(species)
        ],
        axis=0,
    )

    def through(x, rows_of, lanes):
        parts = halves(x)
        return fold(dot(parts, wh_ref[rows_of, lanes])) + dot(
            parts[: x.shape[0]], wl_ref[rows_of, lanes]
        )

    p_own, p_rim = pressure, sent[:rows]
    sum_one = jnp.zeros((rows, ext), F32)
    sum_two = jnp.zeros((rows, ext), F32)
    lap_rim = through(p_own, OWN, RIM)
    pending = []
    for n in range(SUBSTEPS):
        last = n == SUBSTEPS - 1
        now = jnp.concatenate([p_own, halo], axis=1)
        if not last:
            q_rim = q_rim - (lap_rim + through(halo, RIM, RIM))
            p_rim = solve(p_rim - q_rim + force_rim, RIM, inv_ref, a_ref, b_ref)
            pair = jnp.concatenate(
                [
                    pad_rows(p_rim, LANES // 2),
                    pad_rows(pltpu.roll(p_rim, rim - half, 1), LANES // 2),
                ],
                axis=0,
            )
            sends[n] = jnp.transpose(pair)[:hal]
            copies = []
            for k, offset in enumerate(cell_offsets):
                copy = pltpu.make_async_remote_copy(
                    src_ref=sends.at[n, pl.ds(k * slots, half)],
                    dst_ref=recvs.at[n, pl.ds(k * half, half)],
                    send_sem=sends_sem.at[n, k],
                    recv_sem=recvs_sem.at[n, k],
                    device_id=peer(offset),
                    device_id_type=MESH,
                )
                copy.start()
                copies.append(copy)
            pending += copies
        if n == 0:
            q_own = prepare(OWN, area)
            lap_own = through(p_own, OWN, OWN)
            factor_columns(coupling, levels, OWN, inv_ref, a_ref, b_ref)
        q_own = q_own - (lap_own + through(halo, RIM, OWN))
        p_own = solve(p_own - q_own + force_own, OWN, inv_ref, a_ref, b_ref)
        if not last:
            sum_one = sum_one + now
            sum_two = sum_two + (SUBSTEPS - n) * now
            lap = through(p_own, OWN, slice(0, ext))
            lap_own, lap_rim = lap[:, OWN], lap[:, RIM]
            if n == 0:
                trs_ref[...] = pick(tracer_ext, gs_ref[...])
            if n == 1:
                tre_ref[...] = pick(tracer_ext, ge_ref[...])
            if n == SUBSTEPS - 2:
                table = (ge_ref[...].astype(F32) - gs_ref[...].astype(F32)).astype(BF16)
                both = pick(jnp.concatenate([sum_one, sum_two], axis=0), table)
                slope = grad_scale * distance
                flow = velocity - slope * both[:rows]
                gathered = SUBSTEPS * velocity - slope * both[rows:]
                gs_ref[...] = table
            for copy in copies:
                copy.wait_recv()
            both = jnp.transpose(pad_rows(recvs[n], LANES))
            second = both[LANES // 2 : LANES // 2 + rows]
            halo = jnp.where(lane < rim // 2, both[:rows], pltpu.roll(second, rim // 2, 1))
        else:
            p_out[...] = p_own[:levels]
            change = (grad_scale * distance) * pick(now, gs_ref[...])
            u_out[...] = (flow - change)[:levels, :owned]
            mean = (gathered - change) * (1.0 / SUBSTEPS) * length
            ahead = jnp.maximum(mean, 0.0)
            back = jnp.minimum(mean, 0.0)
            for s in range(species):
                part = slice(s * rows, (s + 1) * rows)
                flux = ahead * trs_ref[part] + back * tre_ref[part]
                change = pick(flux, d_ref[:, OWN]) * (tracer_scale * area)
                t_out[s] = (tracers[s] - change)[:levels]
    for copy in first + efirst + pending:
        copy.wait_send()


def write_out(p_in, u_in, t_in, p_out, u_out, t_out, write_sem):
    copies = [
        pltpu.make_async_copy(source, target, write_sem.at[k])
        for k, (source, target) in enumerate(((t_in, t_out), (u_in, u_out), (p_in, p_out)))
    ]
    for copy in copies:
        copy.start()
    for copy in copies:
        copy.wait()


def per_device(
    pressure, velocity, tracers, tendency, pattern, coupling, edge_length, inv_distance,
    inv_area, edge_ends, halo_ends, cell_edges, cell_signs, cell_send, edge_send,
):
    stride = max(4, lax.axis_size("blk") // 16)
    cell_offsets = (1, -1, stride, -stride, stride - 1, 1 - stride)
    edge_offsets = (1, stride, -stride, 1 - stride)
    levels, own = pressure.shape
    species = tracers.shape[0]
    owned = velocity.shape[1]
    peers, slots = cell_send.shape
    epeers, eslots = edge_send.shape
    rows = up_to(levels, 8)
    hal = peers * slots
    rim = up_to(hal, LANES)
    ehal = epeers * eslots
    ext, total = own + rim, owned + ehal
    wide = up_to((species + 1) * rows, LANES)
    steps = len(strides(rows))
    sem = pltpu.SemaphoreType.DMA
    vmem = pl.BlockSpec(memory_space=pltpu.VMEM)
    rounds = SUBSTEPS - 1
    operands = (
        pressure, velocity, tracers, tendency, pattern.reshape(-1, LANES), coupling,
        edge_length.reshape(-1, LANES), inv_distance.reshape(-1, LANES),
        inv_area.reshape(-1, LANES),
        edge_ends, halo_ends, cell_edges, cell_signs, cell_send, edge_send,
    )
    results = pl.pallas_call(
        functools.partial(kernel, cell_offsets, edge_offsets),
        out_shape=(
            pltpu.VMEM(pressure.shape, F32),
            pltpu.VMEM(velocity.shape, F32),
            pltpu.VMEM(tracers.shape, F32),
        ),
        in_specs=[pl.BlockSpec(memory_space=pltpu.HBM)] * 15,
        out_specs=(vmem, vmem, vmem),
        scratch_shapes=[
            pltpu.VMEM((hal, wide), F32),
            pltpu.VMEM((hal, wide), F32),
            pltpu.VMEM((ehal, LANES), F32),
            pltpu.VMEM((ehal, LANES), F32),
            pltpu.VMEM((rounds, hal, LANES), F32),
            pltpu.VMEM((rounds, hal // 2, LANES), F32),
            pltpu.VMEM((ext, total), BF16),
            pltpu.VMEM((ext, total), BF16),
            pltpu.VMEM((2 * ext, total), BF16),
            pltpu.VMEM((total, ext), BF16),
            pltpu.VMEM((ext, ext), BF16),
            pltpu.VMEM((ext, ext), BF16),
            pltpu.VMEM((steps, rows, ext), F32),
            pltpu.VMEM((steps, rows, ext), F32),
            pltpu.VMEM((rows, ext), F32),
            pltpu.VMEM((species * rows, total), F32),
            pltpu.VMEM((species * rows, total), F32),
            pltpu.VMEM(pressure.shape, F32),
            pltpu.VMEM(velocity.shape, F32),
            pltpu.VMEM(tracers.shape, F32),
            pltpu.VMEM(tendency.shape, F32),
            pltpu.VMEM((pattern.shape[0] // LANES, LANES), F32),
            pltpu.VMEM(coupling.shape, F32),
            pltpu.VMEM((owned // LANES, LANES), F32),
            pltpu.VMEM((owned // LANES, LANES), F32),
            pltpu.VMEM((own // LANES, LANES), F32),
            pltpu.VMEM(edge_ends.shape, jnp.int32),
            pltpu.VMEM(halo_ends.shape, jnp.int32),
            pltpu.VMEM(cell_edges.shape, jnp.int32),
            pltpu.VMEM(cell_signs.shape, jnp.int32),
            pltpu.VMEM(cell_send.shape, jnp.int32),
            pltpu.VMEM(edge_send.shape, jnp.int32),
            sem((15,)),
            sem((peers,)),
            sem((peers,)),
            sem((epeers,)),
            sem((epeers,)),
            sem((rounds, peers)),
            sem((rounds, peers)),
        ],
        compiler_params=pltpu.CompilerParams(
            collective_id=0, has_side_effects=True, vmem_limit_bytes=32 * 1024 * 1024
        ),
    )(*[pltpu.with_memory_space_constraint(x, pltpu.HBM) for x in operands])
    anywhere = pl.BlockSpec(memory_space=pl.ANY)
    return pl.pallas_call(
        write_out,
        out_shape=tuple(jax.ShapeDtypeStruct(x.shape, F32) for x in results),
        in_specs=[vmem] * 3,
        out_specs=[anywhere] * 3,
        scratch_shapes=[sem((3,))],
        compiler_params=pltpu.CompilerParams(vmem_limit_bytes=1024 * 1024),
    )(*[pltpu.with_memory_space_constraint(x, pltpu.VMEM) for x in results])


def solution(mesh):
    both = ("member", "blk")
    in_specs = (
        P(None, both), P(None, both), P(None, None, both), P(None, both), P(both),
        P(None, "blk"), P("blk"), P("blk"), P("blk"),
        P(None, "blk"), P(None, "blk"), P(None, "blk"), P(None, "blk"), P(None, "blk"),
        P(None, "blk"),
    )
    out_specs = (P(None, both), P(None, both), P(None, None, both))
    return jax.shard_map(
        per_device, mesh=mesh, in_specs=in_specs, out_specs=out_specs, check_vma=False
    )
```
